32 devices in a mesh: row: 8 (over y, x, core), col: 4 (over z).
Axes of the slice: x: 2, y: 2, z: 4, core: 2. Of those that a mesh axis runs over, the one named last changes fastest.
Arguments:
- source: float32 [512, 512, 512], P('row', 'col'), may hold values from -8 to 8
- basis_x: float32 [512, 512], replicated, may hold values from -0.25 to 0.25
- basis_y: float32 [512, 512], replicated, may hold values from -0.25 to 0.25
- basis_z: float32 [512, 512], replicated, may hold values from -0.25 to 0.25
- eigen_x: float32 [512], replicated, may hold values from 0.1 to 10
- eigen_y: float32 [512], replicated, may hold values from 0.1 to 10
- eigen_z: float32 [512], replicated, may hold values from 0.1 to 10
Outputs:
- solution: float32 [512, 512, 512], P('row', 'col')
The draws below stay inside these ranges and needn't reach their ends.
All inputs are finite; a program needn't handle non-finite values.
Results may differ from the reference program's by a relative error of at most 0.00007.
Values sent between devices are 32-bit elements; how exact they have to be, the bound alone decides.
No kernel may reach another device: no remote copies, remote signals or barrier semaphores. Data moves between devices by JAX's collectives and lax.ppermute only.
A program may use at most 128 MiB of HBM per device.

```python
import math
import jax
import jax.numpy as jnp
from jax import lax

NX = 512
NY = 512
NZ = 512


def levels(stream_key, extent, cuts, smallest, top_value):
    level, own = 1.0, jax.random.fold_in(stream_key, 6)
    for axis_at, parts in cuts:
        draws = jnp.exp(jax.random.uniform(jax.random.fold_in(own, axis_at), (parts,), jnp.float32, smallest / len(cuts), top_value / len(cuts)))
        level = level * jnp.repeat(draws, extent[axis_at] // parts).reshape([-1 if axis == axis_at else 1 for axis in range(len(extent))])
    return level


def gaussian(stream_key, extent, width, limit, split=(), held_as=jnp.bfloat16):
    values = jax.random.normal(stream_key, extent, jnp.float32) * width
    if len(split) > 0:
        values = levels(stream_key, extent, split, -0.22, 0.18) * values
    return jnp.clip(values, min=-limit, max=limit).astype(held_as)


def setup_inputs(seed: int = 0) -> dict:
    keys = jax.random.split(jax.random.key(seed), 8)
    source = gaussian(keys[0], (NX, NY, NZ), 1.0, 8.0, ((0, 8), (1, 4)), jnp.float32)
    basis_x = gaussian(keys[1], (NX, NX), NX ** -0.5, 0.25, (), jnp.float32)
    basis_y = gaussian(keys[2], (NY, NY), NY ** -0.5, 0.25, (), jnp.float32)
    basis_z = gaussian(keys[3], (NZ, NZ), NZ ** -0.5, 0.25, (), jnp.float32)
    eigen_x = jnp.clip(jnp.exp(jax.random.uniform(keys[4], (NX,), jnp.float32, math.log(0.1), math.log(10.0))), 0.1, 10.0)
    eigen_y = jnp.clip(jnp.exp(jax.random.uniform(keys[5], (NY,), jnp.float32, math.log(0.1), math.log(10.0))), 0.1, 10.0)
    eigen_z = jnp.clip(jnp.exp(jax.random.uniform(keys[6], (NZ,), jnp.float32, math.log(0.1), math.log(10.0))), 0.1, 10.0)
    return {"source": source, "basis_x": basis_x, "basis_y": basis_y, "basis_z": basis_z, "eigen_x": eigen_x, "eigen_y": eigen_y, "eigen_z": eigen_z}


HIGH = lax.Precision.HIGHEST


def reference(source, basis_x, basis_y, basis_z, eigen_x, eigen_y, eigen_z):
    field = jnp.einsum('ai,abc->ibc', basis_x, source, precision=HIGH)
    field = jnp.einsum('bj,ibc->ijc', basis_y, field, precision=HIGH)
    field = jnp.einsum('ck,ijc->ijk', basis_z, field, precision=HIGH)
    denom = eigen_x[:, None, None] + eigen_y[None, :, None] + eigen_z[None, None, :]
    field = field / denom
    field = jnp.einsum('ck,ijk->ijc', basis_z, field, precision=HIGH)
    field = jnp.einsum('bj,ijc->ibc', basis_y, field, precision=HIGH)
    field = jnp.einsum('ai,ibc->abc', basis_x, field, precision=HIGH)
    return field
```

```python
import jax
import jax.numpy as jnp
from jax import lax
from jax.experimental import pallas as pl
from jax.experimental.pallas import tpu as pltpu
from jax.sharding import PartitionSpec as P


F32, BF16 = jnp.float32, jnp.bfloat16
CHUNKS = 4
PARTS = 4
LINES = 8
ROWS = 512


def halves(values):
    high = values.astype(BF16)
    return high, (values - high.astype(F32)).astype(BF16)


def product(left, right, dims=((1,), (0,))):
    def one(first, second):
        return lax.dot_general(first, second, (dims, ((), ())), preferred_element_type=F32)

    return one(left[0], right[0]) + (one(left[0], right[1]) + one(left[1], right[0]))


def cost(flops, values):
    return pl.CostEstimate(flops=3 * flops, bytes_accessed=4 * values, transcendentals=0)


def smem():
    return pl.BlockSpec(memory_space=pltpu.SMEM)


def whole(shape):
    return pl.BlockSpec(shape, lambda i: (0,) * len(shape))


def forward_z(basis, source, me, count, planes, chunks, at_line, lines):
    _, width, depth = source.shape
    full = basis.shape[1]
    step = min(LINES, lines)
    own = full // count
    starts = [(shift, chunk * planes) for chunk in chunks for shift in range(count)]
    total = len(starts) * planes

    def kernel(me_ref, basis_ref, source_ref, *refs):
        outs, (turned, high, low) = refs[:-3], refs[-3:]

        @pl.when(pl.program_id(0) == 0)
        def _():
            turned[...] = basis_ref[...].T
            for at, (shift, first) in enumerate(starts):
                block = lax.rem(me_ref[0] + shift, count) * own + first
                block = turned[pl.ds(pl.multiple_of(block, 8), planes), :]
                here = slice(at * planes, (at + 1) * planes)
                high[here], low[here] = halves(block)

        def pair(turn, carry):
            at = turn * 2
            block = source_ref[pl.ds(at, 2)].reshape(2 * width, depth)
            result = product((high[...], low[...]), halves(block), ((1,), (1,)))
            for place, out in enumerate(outs):
                flat = out.reshape(planes * step, width)
                rows = result[place * planes : (place + 1) * planes]
                flat[pl.ds(at, planes, stride=step), :] = rows[:, :width]
                flat[pl.ds(at + 1, planes, stride=step), :] = rows[:, width:]
            return carry

        lax.fori_loop(0, step // 2, pair, 0, unroll=2)

    return pl.pallas_call(
        kernel,
        grid=(lines // step,),
        in_specs=[
            smem(),
            whole((depth, full)),
            pl.BlockSpec((step, width, depth), lambda i: (i + at_line // step, 0, 0)),
        ],
        out_specs=[pl.BlockSpec((planes, step, width), lambda i: (0, i, 0))] * len(starts),
        out_shape=[jax.ShapeDtypeStruct((planes, lines, width), F32)] * len(starts),
        scratch_shapes=[pltpu.VMEM((full, depth), F32)] + [pltpu.VMEM((total, depth), BF16)] * 2,
        cost_estimate=cost(2 * total * lines * width * depth, lines * width * (depth + total)),
        name="forward_z",
    )(me, basis, source)


def prepare_z(basis, me, count):
    depth, full = basis.shape
    own = full // count

    def kernel(me_ref, basis_ref, high, low, turned):
        turned[...] = basis_ref[...].T
        parts = []
        for shift in range(count):
            block = lax.rem(me_ref[0] + (count - shift), count) * own
            parts.append(turned[pl.ds(pl.multiple_of(block, 8), own), :])
        high[...], low[...] = halves(jnp.concatenate(parts, axis=0).T)

    return pl.pallas_call(
        kernel,
        in_specs=[smem(), pl.BlockSpec(memory_space=pltpu.VMEM)],
        out_specs=[pl.BlockSpec(memory_space=pltpu.VMEM)] * 2,
        out_shape=[jax.ShapeDtypeStruct((depth, full), BF16)] * 2,
        scratch_shapes=[pltpu.VMEM((full, depth), F32)],
        cost_estimate=cost(depth * full, 2 * depth * full),
        name="prepare_z",
    )(me, basis)


def backward_z(basis, fields, last, count, total, at_line, result):
    depth, full = basis[0].shape
    planes, lines, width = last[0].shape
    step = min(LINES, lines)
    offset = at_line // step
    earlier = len(fields) // count
    held = [] if result is None else [result]

    def kernel(high, low, *refs):
        out = refs[-1]
        fields, last = refs[: count * earlier], refs[count * earlier : count * (earlier + 1)]

        def pair(turn, carry):
            at = turn * 2
            columns = []
            for line in (at, at + 1):
                parts = []
                for shift in range(count):
                    for ref in (*fields[shift * earlier : (shift + 1) * earlier], last[shift]):
                        parts.append(ref.reshape(planes * step, width)[pl.ds(line, planes, stride=step), :])
                columns.append(jnp.concatenate(parts, axis=0))
            result = product((high[...], low[...]), halves(jnp.concatenate(columns, axis=1)))
            out[at] = result[:, :width].T
            out[at + 1] = result[:, width:].T
            return carry

        lax.fori_loop(0, step // 2, pair, 0, unroll=2)

    return pl.pallas_call(
        kernel,
        grid=(lines // step,),
        in_specs=[whole((depth, full))] * 2
        + [pl.BlockSpec((planes, step, width), lambda i: (0, i + offset, 0))] * len(fields)
        + [pl.BlockSpec((planes, step, width), lambda i: (0, i, 0))] * count
        + [pl.BlockSpec(memory_space=pl.ANY)] * len(held),
        out_specs=pl.BlockSpec((step, width, depth), lambda i: (i + offset, 0, 0)),
        out_shape=jax.ShapeDtypeStruct((total, width, depth), F32),
        input_output_aliases={2 + len(fields) + count: 0} if held else {},
        cost_estimate=cost(2 * lines * width * depth * full, lines * width * (depth + full)),
        name="backward_z",
    )(*basis, *fields, *last, *held)


def y_grid(planes, lines):
    step = min(planes, max(1, ROWS // lines))
    return step, (planes // step,)


def forward_y(basis, fields, me):
    count, pieces = len(fields), len(fields[0])
    planes, piece, width = fields[0][0].shape
    lines = piece * pieces
    full = basis.shape[1]
    step, grid = y_grid(planes, lines)

    def kernel(me_ref, basis_ref, *refs):
        fields, out, high, low = refs[:-3], *refs[-3:]

        @pl.when(pl.program_id(0) == 0)
        def _():
            for shift in range(count):
                block = lax.rem(me_ref[0] + (count - shift), count) * width
                block = basis_ref[pl.ds(pl.multiple_of(block, 8), width), :]
                high[shift * width : (shift + 1) * width], low[shift * width : (shift + 1) * width] = halves(block)

        columns = []
        for shift in range(count):
            parts = [ref[...] for ref in fields[shift * pieces : (shift + 1) * pieces]]
            columns.append(jnp.concatenate(parts, axis=1).reshape(step * lines, width))
        field = jnp.concatenate(columns, axis=1)
        out[...] = product(halves(field), (high[...], low[...])).reshape(step, lines, full)

    return pl.pallas_call(
        kernel,
        grid=grid,
        in_specs=[smem(), whole(basis.shape)]
        + [pl.BlockSpec((step, piece, width), lambda i: (i, 0, 0))] * (count * pieces),
        out_specs=pl.BlockSpec((step, lines, full), lambda i: (i, 0, 0)),
        out_shape=jax.ShapeDtypeStruct((planes, lines, full), F32),
        scratch_shapes=[pltpu.VMEM((count * width, full), BF16)] * 2,
        cost_estimate=cost(2 * planes * lines * width * count * full, planes * lines * (width * count + full)),
        name="forward_y",
    )(me, basis, *[part for parts in fields for part in parts])


def backward_y(basis, field, me, count, pieces):
    planes, lines, full = field.shape
    width = basis.shape[0] // count
    piece = lines // pieces
    step, grid = y_grid(planes, lines)

    def kernel(me_ref, basis_ref, field_ref, *refs):
        outs, (high, low) = refs[:-2], refs[-2:]

        @pl.when(pl.program_id(0) == 0)
        def _():
            for shift in range(count):
                block = lax.rem(me_ref[0] + shift, count) * width
                block = basis_ref[pl.ds(pl.multiple_of(block, 8), width), :]
                high[shift * width : (shift + 1) * width], low[shift * width : (shift + 1) * width] = halves(block)

        field = field_ref[...].reshape(step * lines, full)
        result = product(halves(field), (high[...], low[...]), ((1,), (1,)))
        for shift in range(count):
            block = result[:, shift * width : (shift + 1) * width].reshape(step, lines, width)
            for at in range(pieces):
                outs[at * count + shift][...] = block[:, at * piece : (at + 1) * piece]

    return pl.pallas_call(
        kernel,
        grid=grid,
        in_specs=[smem(), whole(basis.shape), pl.BlockSpec((step, lines, full), lambda i: (i, 0, 0))],
        out_specs=[pl.BlockSpec((step, piece, width), lambda i: (i, 0, 0))] * (count * pieces),
        out_shape=[jax.ShapeDtypeStruct((planes, piece, width), F32)] * (count * pieces),
        scratch_shapes=[pltpu.VMEM((count * width, full), BF16)] * 2,
        cost_estimate=cost(2 * planes * lines * width * count * full, planes * lines * (width * count + full)),
        name="backward_y",
    )(me, basis, field)


def solve_x(field, basis, eigen_x, eigen_y, eigen_z):
    rows, planes, lines, full = field.shape
    nx = basis.shape[0]
    block = pl.BlockSpec((rows, 1, lines, full), lambda p: (0, p, 0, 0))

    def kernel(eig_ref, basis_ref, ex_ref, ey_ref, in_ref, out_ref, plain, turned):
        plane = pl.program_id(0)

        @pl.when(plane == 0)
        def _():
            plain[0], plain[1] = halves(basis_ref[...])
            turned[0], turned[1] = halves(basis_ref[...].T)

        field = in_ref[:, 0].reshape(rows * lines, full)
        field = product((turned[0], turned[1]), halves(field))
        field = field / (ex_ref[...] + ey_ref[...] + eig_ref[plane])
        field = product((plain[0], plain[1]), halves(field))
        out_ref[:, 0] = field.reshape(rows, lines, full)

    return pl.pallas_call(
        kernel,
        grid=(planes,),
        in_specs=[smem(), whole((nx, nx)), whole((nx, 1)), whole((1, full)), block],
        out_specs=block,
        out_shape=jax.ShapeDtypeStruct(field.shape, F32),
        scratch_shapes=[pltpu.VMEM((2, nx, nx), BF16)] * 2,
        cost_estimate=cost(4 * planes * nx * nx * full, 2 * planes * nx * full),
        name="solve_x",
    )(eigen_z, basis, eigen_x[:, None], eigen_y[None, :], field)


def local(source, basis_x, basis_y, basis_z, eigen_x, eigen_y, eigen_z):
    rows, cols = lax.axis_size("row"), lax.axis_size("col")
    row, col = lax.axis_index("row"), lax.axis_index("col")
    lines, _, _ = source.shape
    full = basis_z.shape[1]
    chunks = min(CHUNKS, full // (rows * cols))
    own = full // cols
    planes = own // chunks
    part = planes // rows
    me = jnp.reshape(col, (1,)).astype(jnp.int32)

    def along_col(fields):
        moved = [fields[0]]
        for shift in range(1, cols):
            ring = [(at, (at + shift) % cols) for at in range(cols)]
            moved.append(lax.ppermute(fields[shift], "col", ring))
        return moved

    def along_row(field):
        return lax.all_to_all(field, "row", split_axis=0, concat_axis=0, tiled=True)

    pieces = max(1, min(PARTS, lines // LINES))
    piece = lines // pieces
    first = []
    for at in range(pieces):
        sent = forward_z(basis_z, source, me, cols, planes, [0], at * piece, piece)
        first.append(along_col(sent))
    got = [[[part[shift] for part in first] for shift in range(cols)]]
    if chunks > 1:
        sent = forward_z(basis_z, source, me, cols, planes, range(1, chunks), 0, lines)
        for chunk in range(1, chunks):
            moved = along_col(sent[(chunk - 1) * cols : chunk * cols])
            got.append([[field] for field in moved])
    back = []
    for chunk in range(chunks):
        field = forward_y(basis_y, got[chunk], me)
        field = along_row(field.reshape(rows, part, lines, field.shape[2]))
        eigen = lax.dynamic_slice_in_dim(eigen_z, col * own + chunk * planes + row * part, part, 0)
        field = solve_x(field, basis_x, eigen_x, eigen_y, eigen)
        field = along_row(field)
        field = field.reshape(planes, lines, field.shape[3])
        final = chunk == chunks - 1
        sent = backward_y(basis_y, field, me, cols, pieces if final else 1)
        if not final:
            back.append(along_col(sent))
    fields = [moved[shift] for shift in range(cols) for moved in back]
    result = None
    ready = prepare_z(basis_z, me, cols)
    last = [along_col(sent[at * cols : (at + 1) * cols]) for at in range(pieces)]
    for at in range(pieces):
        result = backward_z(ready, fields, last[at], cols, lines, at * piece, result)
    return result


def solution(mesh):
    placed = (P("row", "col", None), P(), P(), P(), P(), P(), P())
    return jax.shard_map(
        local, mesh=mesh, in_specs=placed, out_specs=P("row", "col", None), check_vma=False
    )
```

```python
import jax
import jax.numpy as jnp
from jax import lax
from jax.experimental import pallas as pl
from jax.experimental.pallas import tpu as pltpu
from jax.sharding import PartitionSpec as P


F32, BF16 = jnp.float32, jnp.bfloat16
CHUNKS = 4
PARTS = 4
LINES = 8
ROWS = 512


def halves(values):
    high = values.astype(BF16)
    return high, (values - high.astype(F32)).astype(BF16)


def product(left, right, dims=((1,), (0,))):
    def one(first, second):
        return lax.dot_general(first, second, (dims, ((), ())), preferred_element_type=F32)

    return one(left[0], right[0]) + (one(left[0], right[1]) + one(left[1], right[0]))


def cost(flops, values):
    return pl.CostEstimate(flops=3 * flops, bytes_accessed=4 * values, transcendentals=0)


def smem():
    return pl.BlockSpec(memory_space=pltpu.SMEM)


def whole(shape):
    return pl.BlockSpec(shape, lambda i: (0,) * len(shape))


def forward_z(basis, source, me, count, planes, chunks, at_line, lines):
    _, width, depth = source.shape
    full = basis.shape[1]
    step = min(LINES, lines)
    own = full // count
    starts = [(shift, chunk * planes) for chunk in chunks for shift in range(count)]
    total = len(starts) * planes

    def kernel(me_ref, basis_ref, source_ref, *refs):
        outs, (turned, high, low) = refs[:-3], refs[-3:]

        @pl.when(pl.program_id(0) == 0)
        def _():
            turned[...] = basis_ref[...].T
            for at, (shift, first) in enumerate(starts):
                block = lax.rem(me_ref[0] + shift, count) * own + first
                block = turned[pl.ds(pl.multiple_of(block, 8), planes), :]
                here = slice(at * planes, (at + 1) * planes)
                high[here], low[here] = halves(block)

        def pair(turn, carry):
            at = turn * 2
            block = source_ref[pl.ds(at, 2)].reshape(2 * width, depth)
            result = product((high[...], low[...]), halves(block), ((1,), (1,)))
            for place, out in enumerate(outs):
                flat = out.reshape(planes * step, width)
                rows = result[place * planes : (place + 1) * planes]
                flat[pl.ds(at, planes, stride=step), :] = rows[:, :width]
                flat[pl.ds(at + 1, planes, stride=step), :] = rows[:, width:]
            return carry

        lax.fori_loop(0, step // 2, pair, 0, unroll=2)

    return pl.pallas_call(
        kernel,
        grid=(lines // step,),
        in_specs=[
            smem(),
            whole((depth, full)),
            pl.BlockSpec((step, width, depth), lambda i: (i + at_line // step, 0, 0)),
        ],
        out_specs=[pl.BlockSpec((planes, step, width), lambda i: (0, i, 0))] * len(starts),
        out_shape=[jax.ShapeDtypeStruct((planes, lines, width), F32)] * len(starts),
        scratch_shapes=[pltpu.VMEM((full, depth), F32)] + [pltpu.VMEM((total, depth), BF16)] * 2,
        cost_estimate=cost(2 * total * lines * width * depth, lines * width * (depth + total)),
        name="forward_z",
    )(me, basis, source)


def prepare_z(basis, me, count):
    depth, full = basis.shape
    own = full // count

    def kernel(me_ref, basis_ref, high, low, turned):
        turned[...] = basis_ref[...].T
        parts = []
        for shift in range(count):
            block = lax.rem(me_ref[0] + (count - shift), count) * own
            parts.append(turned[pl.ds(pl.multiple_of(block, 8), own), :])
        high[...], low[...] = halves(jnp.concatenate(parts, axis=0).T)

    return pl.pallas_call(
        kernel,
        in_specs=[smem(), pl.BlockSpec(memory_space=pltpu.VMEM)],
        out_specs=[pl.BlockSpec(memory_space=pltpu.VMEM)] * 2,
        out_shape=[jax.ShapeDtypeStruct((depth, full), BF16)] * 2,
        scratch_shapes=[pltpu.VMEM((full, depth), F32)],
        cost_estimate=cost(depth * full, 2 * depth * full),
        name="prepare_z",
    )(me, basis)


def backward_z(basis, fields, last, count, total, at_line, result):
    depth, full = basis[0].shape
    planes, lines, width = last[0].shape
    step = min(LINES, lines)
    offset = at_line // step
    earlier = len(fields) // count
    held = [] if result is None else [result]

    def kernel(high, low, *refs):
        out = refs[-1]
        fields, last = refs[: count * earlier], refs[count * earlier : count * (earlier + 1)]

        def pair(turn, carry):
            at = turn * 2
            columns = []
            for line in (at, at + 1):
                parts = []
                for shift in range(count):
                    for ref in (*fields[shift * earlier : (shift + 1) * earlier], last[shift]):
                        parts.append(ref.reshape(planes * step, width)[pl.ds(line, planes, stride=step), :])
                columns.append(jnp.concatenate(parts, axis=0))
            result = product((high[...], low[...]), halves(jnp.concatenate(columns, axis=1)))
            out[at] = result[:, :width].T
            out[at + 1] = result[:, width:].T
            return carry

        lax.fori_loop(0, step // 2, pair, 0, unroll=2)

    return pl.pallas_call(
        kernel,
        grid=(lines // step,),
        in_specs=[whole((depth, full))] * 2
        + [pl.BlockSpec((planes, step, width), lambda i: (0, i + offset, 0))] * len(fields)
        + [pl.BlockSpec((planes, step, width), lambda i: (0, i, 0))] * count
        + [pl.BlockSpec(memory_space=pl.ANY)] * len(held),
        out_specs=pl.BlockSpec((step, width, depth), lambda i: (i + offset, 0, 0)),
        out_shape=jax.ShapeDtypeStruct((total, width, depth), F32),
        input_output_aliases={2 + len(fields) + count: 0} if held else {},
        cost_estimate=cost(2 * lines * width * depth * full, lines * width * (depth + full)),
        name="backward_z",
    )(*basis, *fields, *last, *held)


def y_grid(planes, lines):
    step = min(planes, max(1, ROWS // lines))
    return step, (planes // step,)


def forward_y(basis, fields, me):
    count, pieces = len(fields), len(fields[0])
    planes, _, width = fields[0][0].shape
    sizes = [part.shape[1] for part in fields[0]]
    lines = sum(sizes)
    full = basis.shape[1]
    step, grid = y_grid(planes, lines)

    def kernel(me_ref, basis_ref, *refs):
        fields, out, high, low = refs[:-3], *refs[-3:]

        @pl.when(pl.program_id(0) == 0)
        def _():
            for shift in range(count):
                block = lax.rem(me_ref[0] + (count - shift), count) * width
                block = basis_ref[pl.ds(pl.multiple_of(block, 8), width), :]
                high[shift * width : (shift + 1) * width], low[shift * width : (shift + 1) * width] = halves(block)

        columns = []
        for shift in range(count):
            parts = [ref[...] for ref in fields[shift * pieces : (shift + 1) * pieces]]
            columns.append(jnp.concatenate(parts, axis=1).reshape(step * lines, width))
        field = jnp.concatenate(columns, axis=1)
        out[...] = product(halves(field), (high[...], low[...])).reshape(step, lines, full)

    return pl.pallas_call(
        kernel,
        grid=grid,
        in_specs=[smem(), whole(basis.shape)]
        + [pl.BlockSpec((step, size, width), lambda i: (i, 0, 0)) for size in sizes] * count,
        out_specs=pl.BlockSpec((step, lines, full), lambda i: (i, 0, 0)),
        out_shape=jax.ShapeDtypeStruct((planes, lines, full), F32),
        scratch_shapes=[pltpu.VMEM((count * width, full), BF16)] * 2,
        cost_estimate=cost(2 * planes * lines * width * count * full, planes * lines * (width * count + full)),
        name="forward_y",
    )(me, basis, *[part for parts in fields for part in parts])


def backward_y(basis, field, me, count, sizes):
    planes, lines, full = field.shape
    width = basis.shape[0] // count
    edges = [sum(sizes[:at]) for at in range(len(sizes))]
    step, grid = y_grid(planes, lines)

    def kernel(me_ref, basis_ref, field_ref, *refs):
        outs, (high, low) = refs[:-2], refs[-2:]

        @pl.when(pl.program_id(0) == 0)
        def _():
            for shift in range(count):
                block = lax.rem(me_ref[0] + shift, count) * width
                block = basis_ref[pl.ds(pl.multiple_of(block, 8), width), :]
                high[shift * width : (shift + 1) * width], low[shift * width : (shift + 1) * width] = halves(block)

        field = field_ref[...].reshape(step * lines, full)
        result = product(halves(field), (high[...], low[...]), ((1,), (1,)))
        for shift in range(count):
            block = result[:, shift * width : (shift + 1) * width].reshape(step, lines, width)
            for at, edge in enumerate(edges):
                outs[at * count + shift][...] = block[:, edge : edge + sizes[at]]

    return pl.pallas_call(
        kernel,
        grid=grid,
        in_specs=[smem(), whole(basis.shape), pl.BlockSpec((step, lines, full), lambda i: (i, 0, 0))],
        out_specs=[pl.BlockSpec((step, size, width), lambda i: (i, 0, 0)) for size in sizes for _ in range(count)],
        out_shape=[jax.ShapeDtypeStruct((planes, size, width), F32) for size in sizes for _ in range(count)],
        scratch_shapes=[pltpu.VMEM((count * width, full), BF16)] * 2,
        cost_estimate=cost(2 * planes * lines * width * count * full, planes * lines * (width * count + full)),
        name="backward_y",
    )(me, basis, field)


def solve_x(field, basis, eigen_x, eigen_y, eigen_z):
    rows, planes, lines, full = field.shape
    nx = basis.shape[0]
    block = pl.BlockSpec((rows, 1, lines, full), lambda p: (0, p, 0, 0))

    def kernel(eig_ref, basis_ref, ex_ref, ey_ref, in_ref, out_ref, plain, turned):
        plane = pl.program_id(0)

        @pl.when(plane == 0)
        def _():
            plain[0], plain[1] = halves(basis_ref[...])
            turned[0], turned[1] = halves(basis_ref[...].T)

        field = in_ref[:, 0].reshape(rows * lines, full)
        field = product((turned[0], turned[1]), halves(field))
        field = field / (ex_ref[...] + ey_ref[...] + eig_ref[plane])
        field = product((plain[0], plain[1]), halves(field))
        out_ref[:, 0] = field.reshape(rows, lines, full)

    return pl.pallas_call(
        kernel,
        grid=(planes,),
        in_specs=[smem(), whole((nx, nx)), whole((nx, 1)), whole((1, full)), block],
        out_specs=block,
        out_shape=jax.ShapeDtypeStruct(field.shape, F32),
        scratch_shapes=[pltpu.VMEM((2, nx, nx), BF16)] * 2,
        cost_estimate=cost(4 * planes * nx * nx * full, 2 * planes * nx * full),
        name="solve_x",
    )(eigen_z, basis, eigen_x[:, None], eigen_y[None, :], field)


def piece_sizes(lines):
    units = max(1, lines // LINES)
    count = min(PARTS, units)
    sizes = [units // count] * count
    sizes[-1] += units - sum(sizes)
    if sizes[0] > 1:
        sizes[0], sizes[-1] = sizes[0] - 1, sizes[-1] + 1
    return [size * (lines // units) for size in sizes]


def last_sizes(lines):
    count = max(1, min(PARTS, lines // LINES))
    sizes = [lines // count] * count
    if sizes[-1] >= 2 * LINES:
        sizes[-1:] = [sizes[-1] - LINES, LINES]
    return sizes


def local(source, basis_x, basis_y, basis_z, eigen_x, eigen_y, eigen_z):
    rows, cols = lax.axis_size("row"), lax.axis_size("col")
    row, col = lax.axis_index("row"), lax.axis_index("col")
    lines, _, _ = source.shape
    full = basis_z.shape[1]
    chunks = min(CHUNKS, full // (rows * cols))
    own = full // cols
    planes = own // chunks
    part = planes // rows
    me = jnp.reshape(col, (1,)).astype(jnp.int32)

    def along_col(fields):
        moved = [fields[0]]
        for shift in range(1, cols):
            ring = [(at, (at + shift) % cols) for at in range(cols)]
            moved.append(lax.ppermute(fields[shift], "col", ring))
        return moved

    def along_row(field):
        return lax.all_to_all(field, "row", split_axis=0, concat_axis=0, tiled=True)

    sizes = piece_sizes(lines)
    ends = last_sizes(lines)
    first = []
    for at, size in enumerate(sizes):
        sent = forward_z(basis_z, source, me, cols, planes, [0], sum(sizes[:at]), size)
        first.append(along_col(sent))
    got = [[[part[shift] for part in first] for shift in range(cols)]]
    if chunks > 1:
        sent = forward_z(basis_z, source, me, cols, planes, range(1, chunks), 0, lines)
        for chunk in range(1, chunks):
            moved = along_col(sent[(chunk - 1) * cols : chunk * cols])
            got.append([[field] for field in moved])
    back = []
    for chunk in range(chunks):
        field = forward_y(basis_y, got[chunk], me)
        field = along_row(field.reshape(rows, part, lines, field.shape[2]))
        eigen = lax.dynamic_slice_in_dim(eigen_z, col * own + chunk * planes + row * part, part, 0)
        field = solve_x(field, basis_x, eigen_x, eigen_y, eigen)
        field = along_row(field)
        field = field.reshape(planes, lines, field.shape[3])
        final = chunk == chunks - 1
        sent = backward_y(basis_y, field, me, cols, ends if final else [lines])
        if not final:
            back.append(along_col(sent))
    fields = [moved[shift] for shift in range(cols) for moved in back]
    result = None
    ready = prepare_z(basis_z, me, cols)
    last = [along_col(sent[at * cols : (at + 1) * cols]) for at in range(len(ends))]
    for at in range(len(ends)):
        edge = sum(ends[:at])
        result = backward_z(ready, fields, last[at], cols, lines, edge, result)
    return result


def solution(mesh):
    placed = (P("row", "col", None), P(), P(), P(), P(), P(), P())
    return jax.shard_map(
        local, mesh=mesh, in_specs=placed, out_specs=P("row", "col", None), check_vma=False
    )
```
